32 devices in a mesh: grp: 4 (over x, core), feat: 8 (over z, y).
Axes of the slice: x: 2, y: 2, z: 4, core: 2. Of those that a mesh axis runs over, the one named last changes fastest.
Arguments:
- resid: bfloat16 [4, 128, 4096], P('grp', 'feat'), may hold values from -600 to 600
- norm_gain: float32 [4, 4096], P('grp'), may hold values from 0.25 to 1.75
- w_gate: bfloat16 [4, 4096, 14336], P('grp', None, 'feat'), may hold values from -0.09375 to 0.09375
- w_up: bfloat16 [4, 4096, 14336], P('grp', None, 'feat'), may hold values from -0.09375 to 0.09375
- w_down: bfloat16 [4, 14336, 4096], P('grp', 'feat'), may hold values from -0.046875 to 0.046875
- w_enc: bfloat16 [4, 4096, 16384], P('grp', None, 'feat'), may hold values from -0.09375 to 0.09375
- b_enc: float32 [4, 16384], P('grp', 'feat'), may hold values from -0.8 to 0.2
- w_dec: bfloat16 [4, 16384, 8192], P('grp', 'feat'), may hold values from -0.046875 to 0.046875
- carry_in: float32 [128, 4096], P('feat'), may hold values from -3 to 3
Outputs:
- errors: float32 [4, 128, 4096], P('grp', 'feat')
- forward: float32 [4, 128, 4096], P('grp', 'feat')
The draws below stay inside these ranges and needn't reach their ends.
All inputs are finite; a program needn't handle non-finite values.
Results may differ from the reference program's by a relative error of at most 0.0044.
Values may be sent and summed in bfloat16 or wider, within the bound.
A program may use at most 192 MiB of HBM per device.

```python
import math
import jax
import jax.numpy as jnp
from jax import lax

D = 4096
FF = 14336
F = 16384
TOKENS = 128
LAYERS = 4


def draw_resid(key, part):
    key_base = jax.random.fold_in(key, 11)
    key_rows = jax.random.fold_in(key, 12)
    key_cols = jax.random.fold_in(key, 13)
    row_scale = jnp.exp(jax.random.uniform(key_rows, (LAYERS, TOKENS, 1), jnp.float32, 0.0, math.log(10.0)))
    col_scale = jnp.exp(jax.random.uniform(key_cols, (LAYERS, 1, D), jnp.float32, 0.0, math.log(10.0)))
    entries = jnp.clip(jax.random.normal(key_base, (LAYERS, TOKENS, D), jnp.float32), -5.5, 5.5)
    return (entries * row_scale * col_scale).astype(jnp.bfloat16)


def level_of(stream_key, dims, split, smallest, top_value):
    loudness, own = 1.0, jax.random.fold_in(stream_key, 6)
    for axis_at, blocks in split:
        draws = jnp.exp(jax.random.uniform(jax.random.fold_in(own, axis_at), (blocks,), jnp.float32, smallest / len(split), top_value / len(split)))
        loudness = loudness * jnp.repeat(draws, dims[axis_at] // blocks).reshape([-1 if axis == axis_at else 1 for axis in range(len(dims))])
    return loudness


def gaussian(stream_key, extent, spread, reach, shards=(), dtype=jnp.bfloat16):
    values = spread * jax.random.normal(stream_key, extent, jnp.float32)
    if shards:
        values = values * level_of(stream_key, extent, shards, -0.22, 0.18)
    return jnp.clip(values, -reach, reach).astype(dtype)


def setup_inputs(seed: int = 0) -> dict:
    keys = jax.random.split(jax.random.key(seed), 10)
    resid = draw_resid(jax.random.fold_in(keys[9], 71), 0)
    norm_gain = jnp.clip(1.0 + 0.15 * jax.random.normal(keys[1], (LAYERS, D), jnp.float32), 0.25, 1.75)
    w_gate = gaussian(keys[2], (LAYERS, D, FF), D ** -0.5, 0.09375, ((0, 4), (2, 8)))
    w_up = gaussian(keys[3], (LAYERS, D, FF), D ** -0.5, 0.09375, ((0, 4), (2, 8)))
    w_down = gaussian(keys[4], (LAYERS, FF, D), FF ** -0.5, 0.046875, ((0, 4), (1, 8)))
    w_enc = gaussian(keys[5], (LAYERS, D, F), D ** -0.5, 0.09375, ((0, 4), (2, 8)))
    b_enc = jnp.clip(-0.8 + 1 * jax.random.uniform(keys[6], (LAYERS, F), jnp.float32) ** level_of(keys[6], (LAYERS, F), ((0, 4), (1, 8)), -0.2, 0.2), -0.8, 0.2)
    w_dec = gaussian(keys[7], (LAYERS, F, 2 * D), F ** -0.5, 0.046875, ((0, 4), (1, 8)))
    carry_in = gaussian(keys[8], (TOKENS, D), 0.5, 3.0, ((0, 8),), jnp.float32)
    return dict(resid=resid, norm_gain=norm_gain, w_gate=w_gate, w_up=w_up, w_down=w_down, w_enc=w_enc, b_enc=b_enc, w_dec=w_dec, carry_in=carry_in)


def reference(resid, norm_gain, w_gate, w_up, w_down, w_enc, b_enc, w_dec, carry_in):
    error_list = []
    forward_list = []
    incoming = carry_in.astype(jnp.float32)
    for layer_idx in range(LAYERS):
        stream = resid[layer_idx].astype(jnp.float32)
        inv_rms = lax.rsqrt(lax.optimization_barrier(jnp.mean(stream * stream, axis=1, keepdims=True)) + 1e-05)
        normed = (stream * inv_rms * norm_gain[layer_idx].astype(jnp.float32)).astype(jnp.bfloat16)
        gate_sum = jnp.dot(normed, w_gate[layer_idx], preferred_element_type=jnp.float32)
        up_sum = jnp.dot(normed, w_up[layer_idx], preferred_element_type=jnp.float32)
        hidden = (jax.nn.silu(gate_sum) * up_sum).astype(jnp.bfloat16)
        mlp_out = jnp.dot(hidden, w_down[layer_idx], preferred_element_type=jnp.float32)
        pre_act = jnp.dot(normed, w_enc[layer_idx], preferred_element_type=jnp.float32) + b_enc[layer_idx].astype(jnp.float32)
        features = jax.nn.relu(pre_act).astype(jnp.bfloat16)
        decoded = jnp.dot(features, w_dec[layer_idx], preferred_element_type=jnp.float32)
        err_rows = decoded[:, :D] + incoming - mlp_out
        to_next = decoded[:, D:]
        error_list.append(err_rows)
        forward_list.append(to_next)
        incoming = to_next
    return (jnp.stack(error_list), jnp.stack(forward_list))
```

```python
import functools

import jax
import jax.numpy as jnp
from jax import lax
from jax.experimental import pallas as pl
from jax.experimental.pallas import tpu as pltpu
from jax.sharding import PartitionSpec as P

MESH = pl.DeviceIdType.MESH
F32 = jnp.float32
BF16 = jnp.bfloat16


def chunk_of(width, want):
    size = want
    while size >= 128:
        if width % size == 0:
            return size
        size -= 128
    return width


def loop(count, body):
    if count == 1:
        body(0)
    else:
        lax.fori_loop(0, count, lambda i, c: (body(i), c)[1], 0)


def at(i, size):
    if isinstance(i, int):
        return pl.ds(i * size, size)
    return pl.ds(pl.multiple_of(i * size, size), size)


def kernel(cfg, resid, gain, w_gate, w_up, w_down, w_enc, b_enc, w_dec, carry, err_out, fwd_out,
           gbuf, ubuf, ebuf, dbuf, wbuf, xall, hidden, feats, keep, ysend, yrecv, zsend, zrecv, fsend, inc,
           gsem, usem, esem, dsem, wsem, agz_s, agz_r, agy_s, agy_r, ys_s, ys_r, zs_s, zs_r, fs_s, fs_r):
    G, Z, r, D, gw, ng, ew, ne, cw, nc = cfg
    nq = 2 * nc
    H = Z * r
    me = lax.axis_index("feat")
    g = lax.axis_index("grp")
    z = me // 2
    y = me - 2 * z
    partner = (g, 2 * z + 1 - y)
    sg, se, sd, sw = gbuf.shape[0], ebuf.shape[0], dbuf.shape[0], wbuf.shape[0]

    def peer(d):
        return (g, 2 * lax.rem(z + d, Z) + y)

    def gate_copy(c):
        s = c % sg
        return pltpu.make_async_copy(w_gate.at[0, :, at(c, gw)], gbuf.at[s], gsem.at[s])

    def up_copy(c):
        s = c % sg
        return pltpu.make_async_copy(w_up.at[0, :, at(c, gw)], ubuf.at[s], usem.at[s])

    def enc_copy(c):
        s = c % se
        return pltpu.make_async_copy(w_enc.at[0, :, at(c, ew)], ebuf.at[s], esem.at[s])

    def dec_copy(q):
        s = q % sd
        return pltpu.make_async_copy(w_dec.at[0, :, at((q + nc) % nq, cw)], dbuf.at[s], dsem.at[s])

    def down_copy(c):
        s = c % sw
        return pltpu.make_async_copy(w_down.at[0, :, at(c, cw)], wbuf.at[s], wsem.at[s])

    for c in range(sg):
        gate_copy(c).start()
        up_copy(c).start()
    for c in range(se):
        enc_copy(c).start()

    barrier = pltpu.get_barrier_semaphore()
    pl.semaphore_signal(barrier, inc=1, device_id=partner, device_id_type=MESH)
    for d in range(1, Z):
        pl.semaphore_signal(barrier, inc=1, device_id=peer(d), device_id_type=MESH)

    for near in (g + 1, g + G - 1):
        pl.semaphore_signal(barrier, inc=1, device_id=(lax.rem(near, G), me), device_id_type=MESH)

    stream = resid[0].astype(F32)
    inv_rms = lax.rsqrt(jnp.mean(stream * stream, axis=1, keepdims=True) + 1e-05)
    own = at(z, r)
    xall[own, :] = (stream * inv_rms * gain[...]).astype(BF16)

    pl.semaphore_wait(barrier, Z + 2)

    def rows_z(d):
        return at(lax.rem(z + Z - d, Z), r)

    def ag_z(d):
        return pltpu.make_async_remote_copy(
            src_ref=xall.at[own], dst_ref=xall.at[own], send_sem=agz_s.at[d - 1], recv_sem=agz_r.at[d - 1],
            device_id=peer(d), device_id_type=MESH)

    def ag_y(d):
        src = lax.rem(z + Z - d, Z)
        return pltpu.make_async_remote_copy(
            src_ref=xall.at[at(src, r)], dst_ref=xall.at[at(Z + src, r)], send_sem=agy_s.at[d], recv_sem=agy_r.at[d],
            device_id=partner, device_id_type=MESH)

    def ag_z_in(d):
        return pltpu.make_async_remote_copy(
            src_ref=xall.at[rows_z(d)], dst_ref=xall.at[rows_z(d)], send_sem=agz_s.at[d - 1], recv_sem=agz_r.at[d - 1],
            device_id=peer(d), device_id_type=MESH)

    for d in range(1, Z):
        ag_z(d).start()
    ag_y(0).start()
    for q in range(sd):
        dec_copy(q).start()
    for c in range(sw):
        down_copy(c).start()
    for d in range(1, Z):
        ag_z_in(d).wait_recv()
        ag_y(d).start()
    for d in range(Z):
        ag_y(d).wait_recv()

    def gate_up(c):
        gate_copy(c).wait()
        up_copy(c).wait()
        s = c % sg
        x = xall[...]
        gate = jnp.dot(x, gbuf[s], preferred_element_type=F32)
        up = jnp.dot(x, ubuf[s], preferred_element_type=F32)
        hidden[:, at(c, gw)] = (jax.nn.silu(gate) * up).astype(BF16)
        if ng > sg:
            @pl.when(c + sg < ng)
            def _():
                gate_copy(c + sg).start()
                up_copy(c + sg).start()

    def encode(c):
        enc_copy(c).wait()
        pre = jnp.dot(xall[...], ebuf[c % se], preferred_element_type=F32) + b_enc[:, at(c, ew)]
        feats[:, at(c, ew)] = jnp.maximum(pre, 0.0).astype(BF16)
        if ne > se:
            @pl.when(c + se < ne)
            def _():
                enc_copy(c + se).start()

    loop(ng, gate_up)
    loop(ne, encode)

    def y_copy(q):
        return pltpu.make_async_remote_copy(
            src_ref=ysend.at[q], dst_ref=yrecv.at[q], send_sem=ys_s.at[q], recv_sem=ys_r.at[q],
            device_id=partner, device_id_type=MESH)

    def z_copy(q, d):
        return pltpu.make_async_remote_copy(
            src_ref=zsend.at[q, at(lax.rem(z + d, Z), r)], dst_ref=zrecv.at[q, d - 1],
            send_sem=zs_s.at[q, d - 1], recv_sem=zs_r.at[q, d - 1], device_id=peer(d), device_id_type=MESH)

    def f_copy(c):
        return pltpu.make_async_remote_copy(
            src_ref=fsend.at[c], dst_ref=inc.at[c], send_sem=fs_s.at[c], recv_sem=fs_r.at[c],
            device_id=(lax.rem(g + 1, G), me), device_id_type=MESH)

    def split_out(q, part):
        keep[q] = part[:H]
        ysend[q] = part[H:].astype(BF16)
        y_copy(q).start()

    def produce(q):
        dec_copy(q).wait()
        part = jnp.dot(feats[...], dbuf[q % sd], preferred_element_type=F32)

        @pl.when(q < nc)
        def _():
            split_out(q, part)

        @pl.when(q >= nc)
        def _():
            c = q - nc
            down_copy(c).wait()
            split_out(q, part - jnp.dot(hidden[...], wbuf[c % sw], preferred_element_type=F32))

            @pl.when(c + sw < nc)
            def _():
                down_copy(c + sw).start()

        @pl.when(q + sd < nq)
        def _():
            dec_copy(q + sd).start()

    def pass_on(q):
        y_copy(q).wait_recv()
        both = keep[q] + yrecv[q].astype(F32)
        keep[q] = both
        zsend[q] = both.astype(BF16)
        for d in range(1, Z):
            z_copy(q, d).start()

    def finish(q):
        total = keep[q, own, :]
        for d in range(1, Z):
            z_copy(q, d).wait_recv()
            total = total + zrecv[q, d - 1].astype(F32)

        @pl.when(q < nc)
        def _():
            fwd_out[0, :, at(q, cw)] = total

            @pl.when(g < G - 1)
            def _():
                fsend[q] = total
                f_copy(q).start()

        @pl.when(q >= nc)
        def _():
            c = q - nc

            @pl.when(g == 0)
            def _():
                err_out[0, :, at(c, cw)] = total + carry[:, at(c, cw)]

            @pl.when(g > 0)
            def _():
                f_copy(c).wait_recv()
                err_out[0, :, at(c, cw)] = total + inc[c]

    lag_z, lag_f = 2, 4

    def step(t):
        @pl.when(t < nq)
        def _():
            produce(t)

        @pl.when((t >= lag_z) & (t < nq + lag_z))
        def _():
            pass_on(t - lag_z)

        @pl.when(t >= lag_f)
        def _():
            finish(t - lag_f)

    loop(nq + lag_f, step)

    for d in range(1, Z):
        ag_z(d).wait_send()
    for d in range(Z):
        ag_y(d).wait_send()

    def drain(q):
        y_copy(q).wait_send()
        for d in range(1, Z):
            z_copy(q, d).wait_send()

        @pl.when((q < nc) & (g < G - 1))
        def _():
            f_copy(q).wait_send()

    loop(nq, drain)


def solution(mesh):
    G, n = mesh.shape["grp"], mesh.shape["feat"]
    Z = n // 2

    def body(resid, norm_gain, w_gate, w_up, w_down, w_enc, b_enc, w_dec, carry_in):
        _, r, D = resid.shape
        fw, en = w_gate.shape[2], w_enc.shape[2]
        gw, ew = chunk_of(fw, 256), chunk_of(en, 256)
        ng, ne = fw // gw, en // ew
        cw = chunk_of(D, 512 if n <= 8 else 2048)
        nc = D // cw
        nq = 2 * nc
        H, T = Z * r, 2 * Z * r
        sg, se, sd, sw = min(4, ng), min(6, ne), min(6, nq), min(4, nc)
        cfg = (G, Z, r, D, gw, ng, ew, ne, cw, nc)
        vm = pl.BlockSpec(memory_space=pltpu.VMEM)
        hbm = pl.BlockSpec(memory_space=pl.ANY)
        sem = lambda *s: pltpu.SemaphoreType.DMA(s)
        return pl.pallas_call(
            functools.partial(kernel, cfg),
            out_shape=(jax.ShapeDtypeStruct((1, r, D), F32), jax.ShapeDtypeStruct((1, r, D), F32)),
            in_specs=[vm, vm, hbm, hbm, hbm, hbm, vm, hbm, vm],
            out_specs=(vm, vm),
            scratch_shapes=[
                pltpu.VMEM((sg, D, gw), BF16),
                pltpu.VMEM((sg, D, gw), BF16),
                pltpu.VMEM((se, D, ew), BF16),
                pltpu.VMEM((sd, en, cw), BF16),
                pltpu.VMEM((sw, fw, cw), BF16),
                pltpu.VMEM((T, D), BF16),
                pltpu.VMEM((T, fw), BF16),
                pltpu.VMEM((T, en), BF16),
                pltpu.VMEM((nq, H, cw), F32),
                pltpu.VMEM((nq, H, cw), BF16),
                pltpu.VMEM((nq, H, cw), BF16),
                pltpu.VMEM((nq, H, cw), BF16),
                pltpu.VMEM((nq, Z - 1, r, cw), BF16),
                pltpu.VMEM((nc, r, cw), F32),
                pltpu.VMEM((nc, r, cw), F32),
                sem(sg), sem(sg), sem(se), sem(sd), sem(sw),
                sem(Z - 1), sem(Z - 1), sem(Z), sem(Z),
                sem(nq), sem(nq), sem(nq, Z - 1), sem(nq, Z - 1), sem(nc), sem(nc),
            ],
            compiler_params=pltpu.CompilerParams(
                collective_id=0, has_side_effects=True, vmem_limit_bytes=67043328),
        )(resid, norm_gain, w_gate, w_up, w_down, w_enc, b_enc, w_dec, carry_in)

    return jax.shard_map(
        body,
        mesh=mesh,
        in_specs=(
            P("grp", "feat", None),
            P("grp", None),
            P("grp", None, "feat"),
            P("grp", None, "feat"),
            P("grp", "feat", None),
            P("grp", None, "feat"),
            P("grp", "feat"),
            P("grp", "feat", None),
            P("feat", None),
        ),
        out_specs=(P("grp", "feat", None), P("grp", "feat", None)),
        check_vma=False,
    )
```
